32 devices in a mesh: row: 4 (over y, core), col: 8 (over z, x).
Axes of the slice: x: 2, y: 2, z: 4, core: 2. Of those that a mesh axis runs over, the one named last changes fastest.
Arguments:
- upper_a: bfloat16 [2, 2048, 4096], P(None, 'row', 'col'), may hold values from -0.125 to 0.125
- upper_b: bfloat16 [4, 2048, 2, 4096], P(None, 'row', None, 'col'), may hold values from -0.125 to 0.125
- right_side: bfloat16 [2, 2048, 2, 4096], P(None, 'row', None, 'col'), may hold values from -6 to 6
- a_bases: bfloat16 [2, 2048, 512], P(None, 'row'), may hold values from -1 to 1, as said below
- b_bases: bfloat16 [2, 4096, 512], P(None, 'col'), may hold values from -1 to 1, as said below
- a_values: float32 [2, 2048], P(None, 'row'), may hold values from 0.25 to 4
- b_values: float32 [2, 4096], P(None, 'col'), may hold values from 0.25 to 4
Outputs:
- solution: float32 [2, 2048, 2, 4096], P(None, 'row', None, 'col')
The draws below stay inside these ranges and needn't reach their ends.
Inputs may be any that keep to these rules, and one draw needn't show every extreme that they name: Each tile of a_bases is an orthonormal matrix rounded to bfloat16. Each tile of b_bases is an orthonormal matrix rounded to bfloat16.
All inputs are finite; a program needn't handle non-finite values.
Results may differ from the reference program's by a relative error of at most 0.012.
Values may be sent and summed in bfloat16 or wider, within the bound.
No kernel may reach another device: no remote copies, remote signals or barrier semaphores. Data moves between devices by JAX's collectives and lax.ppermute only.
A program may use at most 128 MiB of HBM per device.

```python
import math
import jax
import jax.numpy as jnp
from jax import lax

NB = 512
CT = 2
FRONTS = 4
TR = 8
RT = 2
TC = 16
BR = 4
M = 4096
FIRST = 6
N_ROW = 4
N_COL = 8


def orthonormal(key, tile_count):
    samples = jax.random.normal(key, (tile_count, NB, NB), jnp.float32)
    factor, triangle = jnp.linalg.qr(samples)
    return factor


def draw_a_bases(key, part):
    return orthonormal(jax.random.fold_in(key, 11), TR).reshape(RT, N_ROW * NB, NB).astype(jnp.bfloat16)


def draw_b_bases(key, part):
    return orthonormal(jax.random.fold_in(key, 23), TC).reshape(CT, N_COL * NB, NB).astype(jnp.bfloat16)


def level_of(stream_key, dims, pieces, low, largest):
    level = 1.0
    for dim, blocks in pieces:
        draws = jax.random.uniform(jax.random.fold_in(jax.random.fold_in(stream_key, 6), dim), (blocks,), jnp.float32, low / len(pieces), largest / len(pieces))
        level = level * jnp.repeat(jnp.exp(draws), dims[dim] // blocks).reshape((-1,) + (1,) * (len(dims) - 1 - dim))
    return level


def normal_values(own_key, extent, spread, limit, pieces=(), kind=jnp.bfloat16):
    result = spread * jax.random.normal(own_key, extent, jnp.float32)
    if pieces:
        result = result * level_of(own_key, extent, pieces, -0.22, 0.18)
    return jnp.clip(result, -limit, limit).astype(kind)


def setup_inputs(seed: int = 0) -> dict:
    streams_of = jax.random.split(jax.random.key(seed), 8)
    return {
        "upper_a": normal_values(streams_of[0], (RT, N_ROW * NB, M), (4 * NB) ** -0.5, 0.125, ((1, 4), (2, 8))),
        "upper_b": normal_values(streams_of[1], (BR, N_ROW * NB, CT, N_COL * NB), (4 * NB) ** -0.5, 0.125, ((1, 4), (3, 8))),
        "right_side": normal_values(streams_of[2], (RT, N_ROW * NB, CT, N_COL * NB), 1.0, 6.0, ((1, 4), (3, 8))),
        "a_bases": draw_a_bases(jax.random.fold_in(streams_of[7], 71), 0),
        "b_bases": draw_b_bases(jax.random.fold_in(streams_of[7], 71), 0),
        "a_values": jnp.clip(jnp.exp(math.log(4.0) - 2.7725887 * jax.random.uniform(streams_of[5], (RT, N_ROW * NB), jnp.float32) ** level_of(streams_of[5], (RT, N_ROW * NB), ((1, 4),), -0.2, 0.2)), 0.25, 4.0),
        "b_values": jnp.clip(jnp.exp(math.log(4.0) - 2.7725887 * jax.random.uniform(streams_of[6], (CT, N_COL * NB), jnp.float32) ** level_of(streams_of[6], (CT, N_COL * NB), ((1, 8),), -0.2, 0.2)), 0.25, 4.0),
    }


def rounded_copy(value):
    return lax.optimization_barrier(value.astype(jnp.bfloat16)).astype(jnp.float32)

def solve_tiles(waiting, basis_left, values_left, basis_right, values_right):
    highest = lax.Precision.HIGHEST
    left_full = basis_left.astype(jnp.float32)
    right_full = basis_right.astype(jnp.float32)
    rounded = rounded_copy(waiting)
    first_half = rounded_copy(jnp.einsum('npq,npr->nqr', left_full, rounded, precision=highest))
    scaled = jnp.einsum('nqr,nrs->nqs', first_half, right_full, precision=highest)
    scaled = rounded_copy(scaled / (values_left[:, :, None] + values_right[:, None, :]))
    left_side = rounded_copy(jnp.einsum('npq,nqs->nps', left_full, scaled, precision=highest))
    return jnp.einsum('nps,nts->npt', left_side, right_full, precision=highest).astype(jnp.bfloat16)

def reference(upper_a, upper_b, right_side, a_bases, b_bases, a_values, b_values):
    highest = lax.Precision.HIGHEST
    working = right_side.astype(jnp.float32).reshape(TR, NB, TC, NB)
    matrix_a = upper_a.astype(jnp.float32).reshape(TR, NB, TR, NB)
    matrix_b = upper_b.astype(jnp.float32).reshape(TC, NB, TC, NB)
    bases_left = a_bases.reshape(TR, NB, NB)
    bases_right = b_bases.reshape(TC, NB, NB)
    values_left = a_values.reshape(TR, NB)
    values_right = b_values.reshape(TC, NB)
    tile_i = jnp.arange(TR, dtype=jnp.int32)
    tile_j = jnp.arange(TC, dtype=jnp.int32)
    for front_step in range(FRONTS):
        front_id = FIRST + front_step
        k_glob = TR - 1 - front_id + tile_j
        k_valid = (k_glob >= 0) & (k_glob <= TR - 1)
        k_safe = jnp.clip(k_glob, 0, TR - 1)
        waiting = working[k_safe, :, tile_j, :]
        solved = solve_tiles(waiting, bases_left[k_safe], values_left[k_safe], bases_right, values_right)
        solved = jnp.where(k_valid[:, None, None], solved, jnp.zeros_like(solved))
        solved_full = solved.astype(jnp.float32)
        working = working.at[k_safe, :, tile_j, :].set(jnp.where(k_valid[:, None, None], solved_full, waiting))
        column_terms = jnp.einsum('ipjq,jqr->ipjr', matrix_a[:, :, k_safe, :], solved_full, precision=highest)
        column_mask = (k_valid[None, :] & (tile_i[:, None] < k_glob[None, :])).astype(jnp.float32)
        l_glob = front_id - TR + 1 + tile_i
        l_safe = jnp.clip(l_glob, 0, TC - 1)
        row_terms = jnp.einsum('ipq,iqjr->ipjr', solved_full[l_safe], matrix_b[l_safe], precision=highest)
        row_mask = ((l_glob[:, None] >= 0) & (l_glob[:, None] < tile_j[None, :])).astype(jnp.float32)
        working = working - column_terms * column_mask[:, None, :, None] - row_terms * row_mask[:, None, :, None]
    return working.reshape(RT, N_ROW * NB, CT, N_COL * NB)
```

```python
import functools

import jax
import jax.numpy as jnp
import numpy as np
from jax import lax
from jax.experimental import pallas as pl
from jax.experimental.pallas import tpu as pltpu
from jax.sharding import PartitionSpec as P

FRONTS = 4
AXES = ("row", "col")
ANY = pl.BlockSpec(memory_space=pl.ANY)
SMEM = pl.BlockSpec(memory_space=pltpu.SMEM)
F32 = jnp.float32
BF16 = jnp.bfloat16


def send(block, pairs):
    return lax.ppermute(block, AXES, sorted(pairs))


class Plan:
    def __init__(self, R, N, a_count, b_count, b_rows):
        self.R, self.N = R, N
        self.a_count, self.b_count, self.b_rows = a_count, b_count, b_rows
        self.pairs_of_rows = R == 4
        half = N // 2
        self.ring = [2 * i for i in range(half)] + [2 * i + 1 for i in reversed(range(half))]
        self.pos = {c: p for p, c in enumerate(self.ring)}
        self.forward = N // 2
        self.backward = N - 1 - self.forward

    def dev(self, r, c):
        return (r % self.R) * self.N + c % self.N

    def sources(self, s):
        for k in range(self.N):
            j = k + s - 1
            if j >= 0:
                yield k, k % self.R, j % self.N

    def column_needs(self, row, k):
        return row < k

    def a_pairs(self, s, a):
        out = []
        for r in range(self.R):
            for c in range(self.N):
                if s == 0 and c == 0:
                    continue
                if r + self.R * a < c:
                    out.append((self.dev(r, c), self.dev(r, c + s - 1)))
        return out

    def b_reads(self, r, c):
        got = set()
        for s in range(FRONTS):
            for a in range(self.a_count):
                l = r + self.R * a - 1 + s
                for b in range(self.b_count):
                    if 0 <= l < c + self.N * b:
                        got.add((l % self.R, l // self.R, b))
        return got

    def b_tiles(self):
        got = set()
        for r in range(self.R):
            for c in range(self.N):
                got |= {(a, b) for _, a, b in self.b_reads(r, c)}
        return sorted(got, key=lambda t: (t[1], -t[0]))


def pick_start(cands, which, dst, sem):
    if len(cands) == 1:
        pltpu.make_async_copy(cands[0], dst, sem).start()
        return
    for n, cand in enumerate(cands):
        @pl.when(which == n)
        def _(cand=cand):
            pltpu.make_async_copy(cand, dst, sem).start()


def pick_wait(cands, dst, sem):
    pltpu.make_async_copy(cands[0], dst, sem).wait()


def dot(x, y):
    return jnp.dot(x, y, preferred_element_type=F32)


class Kernel:
    def __init__(self):
        self.arrays, self.ids = [], {}

    def add(self, array):
        if id(array) not in self.ids:
            self.ids[id(array)] = len(self.arrays)
            self.arrays.append(array)
        return self.ids[id(array)]

    def cand(self, array, *index):
        return (self.add(array), index)


def at(refs, cand):
    n, index = cand
    return refs[n].at[index] if index else refs[n]


def call(body, kernel, table, out_shape, scratch, flops, name, aliases=None):
    n = len(kernel.arrays)

    def wrapped(table_ref, *rest):
        body(table_ref, rest[:n], rest[n], *rest[n + 1:])

    return pl.pallas_call(
        wrapped,
        out_shape=out_shape,
        in_specs=[SMEM] + [ANY] * n,
        out_specs=ANY,
        scratch_shapes=scratch,
        input_output_aliases=aliases or {},
        cost_estimate=pl.CostEstimate(flops=flops, bytes_accessed=1 << 22, transcendentals=0),
        name=name,
    )(table, *kernel.arrays)


def shards(upper_a, upper_b, right_side, a_bases, b_bases, a_values, b_values):
    R = lax.axis_size("row")
    N = lax.axis_size("col")
    A_CNT, B_CNT, B_ROWS = right_side.shape[0], right_side.shape[2], upper_b.shape[0]
    nb = right_side.shape[1]
    plan = Plan(R, N, A_CNT, B_CNT, B_ROWS)
    dev = plan.dev
    tile = (nb, nb)
    mm = 2 * nb**3

    columns = {}

    def column(name, fn):
        columns[name] = np.array([fn(r, c) for r in range(R) for c in range(N)], np.int32)

    def own(r, c):
        s = (c - r + 1) % R
        if s >= FRONTS:
            return None
        k = (c - s + 1)
        if k >= N:
            return None
        b = 0
        if k < 0:
            k, b = k + N, 1
        return s, k, k // R, b

    column("a0", lambda r, c: (own(r, c) or (0, 0, 0, 0))[2])
    column("b0", lambda r, c: (own(r, c) or (0, 0, 0, 0))[3])
    column("s0", lambda r, c: (own(r, c) or (FRONTS, 0, 0, 0))[0])
    for a in range(A_CNT):
        for b in range(B_CNT):
            column(f"active{a}{b}", lambda r, c: int(c + N * b > r + R * a + FRONTS - 2))
            column(
                f"own{a}{b}",
                lambda r, c: int(own(r, c) is not None and own(r, c)[2:] == (a, b)),
            )
    for s in range(FRONTS):
        for b in range(B_CNT):
            def col_valid(r, c):
                k = c - s + 1
                return int(k < N and (0 if k >= 0 else 1) == b)
            column(f"col{s}{b}", col_valid)

    for t in range(FRONTS - 1):
        column(
            f"below{t}",
            lambda r, c: int(
                own(r, c) is not None and own(r, c)[0] > t and own(r, c)[1] + own(r, c)[0] - t < N
            ),
        )

    a_moved = {}
    for s in range(FRONTS):
        a_moved[s] = [None] * A_CNT
    for a in range(A_CNT):
        a_moved[0][a] = send(upper_a[a], plan.a_pairs(0, a))

    tiles = plan.b_tiles()
    b_rows = 1 + max(a for a, _ in tiles)
    b_stack = jnp.transpose(upper_b[:b_rows], (0, 2, 1, 3))
    c_stack = jnp.transpose(right_side, (0, 2, 1, 3))

    b_from = {}
    home = {t: (b_stack, t) for t in tiles}

    def b_cross_needed(r, c, t):
        return any((r, *t) in plan.b_reads(d, c) for d in (r ^ 2, r ^ 3))

    if plan.pairs_of_rows:
        mates = [(dev(r, c), dev(r ^ 1, c)) for r in range(R) for c in range(N)]
        mate_stack = send(b_stack, mates)
        mate = {t: (mate_stack, t) for t in tiles}
        across, across_mate = {}, {}
        for t in tiles:
            moved = send(
                b_stack[t],
                [
                    (dev(r, c), dev(r ^ 2, c))
                    for r in range(R)
                    for c in range(N)
                    if b_cross_needed(r, c, t)
                ],
            )
            across[t] = (moved, ())
            across_mate[t] = (
                send(
                    moved,
                    [
                        (dev(r, c), dev(r ^ 1, c))
                        for r in range(R)
                        for c in range(N)
                        if (r ^ 2, *t) in plan.b_reads(r ^ 1, c)
                    ],
                ),
                (),
            )

        def b_source(r, src, t):
            return {0: home, 1: mate, 2: across, 3: across_mate}[r ^ src].get(t)
    else:
        shifted = {1: home}
        for s in (0, 2, 3):
            moved = send(
                b_stack, [(dev(r + s - 1, c), dev(r, c)) for r in range(R) for c in range(N)]
            )
            shifted[s] = {t: (moved, t) for t in tiles}

        def b_source(r, src, t):
            return shifted[(src - r + 1) % R].get(t)

    def b_cands(name, s, reads):
        cands, keys, choice = [], {}, []
        for r in range(R):
            for c in range(N):
                n = 0
                ab = reads(r, c)
                if ab is not None:
                    a, b = ab
                    l = r + R * a - 1 + s
                    if 0 <= l < c + N * b:
                        cand = b_source(r, l % R, (l // R, b))
                        key = (id(cand[0]), cand[1])
                        if key not in keys:
                            keys[key] = len(cands)
                            cands.append(cand)
                        n = keys[key]
                choice.append(n)
        columns[name] = np.array(choice, np.int32)
        return cands

    own_b = {}
    for s in range(FRONTS - 1):
        def reads(r, c, s=s):
            o = own(r, c)
            return o[2:] if o is not None and o[0] > s else None
        own_b[s] = b_cands(f"ownb{s}", s, reads)
    all_b = {}
    for s in range(FRONTS):
        for a in range(A_CNT):
            for b in range(B_CNT):
                def reads(r, c, a=a, b=b):
                    return (a, b) if c + N * b > r + R * a + FRONTS - 2 else None
                all_b[s, a, b] = b_cands(f"b{s}{a}{b}", s, reads)
    for s in range(FRONTS):
        for a in range(A_CNT):
            def row_pick(r, c):
                k = r + R * a
                if k + s - 1 < 0:
                    return 0
                dist = (plan.pos[c] - plan.pos[(k + s - 1) % N]) % N
                return dist if dist <= plan.forward else plan.forward + N - dist
            column(f"xr{s}{a}", row_pick)
            column(f"rowok{s}{a}", lambda r, c: int(r + R * a + s - 1 >= 0))
        def col_pick(r, c):
            k = (c - s + 1) % N
            off = (k - r) % R
            if off == 0:
                return 0
            if not plan.pairs_of_rows:
                return off
            if off == 1:
                return 1
            odd = k % 2
            return (2 if odd else 3) if off == 2 else (3 if odd else 2)
        column(f"xc{s}", col_pick)

    names = list(columns)
    where = {name: n for n, name in enumerate(names)}
    table = jnp.asarray(np.stack([columns[n] for n in names], 1))
    me = lax.axis_index("row") * N + lax.axis_index("col")
    table = lax.dynamic_slice_in_dim(table, me, 1, 0)[0]
    a0, b0 = table[where["a0"]], table[where["b0"]]
    denominators = (
        lax.dynamic_index_in_dim(a_values, a0, 0, False)[:, None]
        + lax.dynamic_index_in_dim(b_values, b0, 0, False)[None, :]
    )

    def solve(s, base, base_index, pairs):
        kernel = Kernel()
        base_c = kernel.cand(base)
        qa_c, qb_c, d_c = kernel.cand(a_bases), kernel.cand(b_bases), kernel.cand(denominators)
        steps = []
        for left_a, xc, xr, bs, lag_s in pairs:
            steps.append(
                (
                    [kernel.cand(*x) for x in left_a],
                    kernel.cand(xc),
                    kernel.cand(xr),
                    [kernel.cand(x[0], *x[1]) for x in bs],
                    lag_s,
                )
            )

        def body(tab, refs, out, base_v, qa, qb, den, xa, xb, xc_v, xr_v, y, sems):
            ia, ib = tab[where["a0"]], tab[where["b0"]]
            src = at(refs, base_c)
            copies = [
                pltpu.make_async_copy(src.at[ia, ib] if base_index else src, base_v, sems.at[0]),
                pltpu.make_async_copy(at(refs, qa_c).at[ia], qa, sems.at[1]),
                pltpu.make_async_copy(at(refs, qb_c).at[ib], qb, sems.at[2]),
                pltpu.make_async_copy(at(refs, d_c), den, sems.at[3]),
            ]
            if steps:
                left_a, xc, xr, bs, lag_s = steps[0]
                la = [at(refs, x) for x in left_a]
                lb = [at(refs, x) for x in bs]
                pick_start(la, ia, xa, sems.at[4])
                pltpu.make_async_copy(at(refs, xc), xc_v, sems.at[5]).start()
                pltpu.make_async_copy(at(refs, xr), xr_v, sems.at[6]).start()
                pick_start(lb, tab[where[f"ownb{lag_s}"]], xb, sems.at[7])
            for cp in copies:
                cp.start()
            if steps:
                pick_wait(la, xa, sems.at[4])
                pltpu.make_async_copy(at(refs, xc), xc_v, sems.at[5]).wait()
                copies[0].wait()

                @pl.when(tab[where[f"below{lag_s}"]] == 0)
                def _():
                    xc_v[...] = jnp.zeros_like(xc_v)

                acc = base_v[...].astype(F32) - dot(xa[...], xc_v[...])
                pltpu.make_async_copy(at(refs, xr), xr_v, sems.at[6]).wait()
                pick_wait(lb, xb, sems.at[7])
                y[...] = (acc - dot(xr_v[...], xb[...])).astype(BF16)
            else:
                copies[0].wait()
                y[...] = base_v[...].astype(BF16)
            copies[1].wait()
            y[...] = lax.dot_general(
                qa[...], y[...], (((0,), (0,)), ((), ())), preferred_element_type=F32
            ).astype(BF16)
            copies[2].wait()
            copies[3].wait()
            y[...] = (dot(y[...], qb[...]) / den[...]).astype(BF16)
            y[...] = dot(qa[...], y[...]).astype(BF16)
            y[...] = lax.dot_general(
                y[...], qb[...], (((1,), (1,)), ((), ())), preferred_element_type=F32
            ).astype(BF16)
            last = pltpu.make_async_copy(y, out, sems.at[0])
            last.start()
            last.wait()

        scratch = [
            pltpu.VMEM(tile, base.dtype),
            pltpu.VMEM(tile, BF16),
            pltpu.VMEM(tile, BF16),
            pltpu.VMEM(tile, F32),
        ] + [pltpu.VMEM(tile, BF16)] * 5 + [pltpu.SemaphoreType.DMA((8,))]
        return call(
            body, kernel, table, jax.ShapeDtypeStruct(tile, BF16), scratch,
            (4 + 2 * len(steps)) * mm, f"solve{s}",
        )

    def older(s, terms):
        kernel = Kernel()
        base_c = kernel.cand(c_stack)
        steps = []
        for left_a, xcs, xc_which, xr, bs, lag_s in terms:
            steps.append(
                (
                    [kernel.cand(*x) for x in left_a],
                    [kernel.cand(x) for x in xcs],
                    xc_which,
                    kernel.cand(xr),
                    [kernel.cand(x[0], *x[1]) for x in bs],
                    lag_s,
                )
            )

        def body(tab, refs, out, base_v, xa, xb, xc_v, xr_v, acc, sems):
            ia, ib = tab[where["a0"]], tab[where["b0"]]
            first = pltpu.make_async_copy(at(refs, base_c).at[ia, ib], base_v, sems.at[0])
            first.start()
            waits = []
            for n, (left_a, xcs, xc_which, xr, bs, lag_s) in enumerate(steps):
                la = [at(refs, x) for x in left_a]
                lc = [at(refs, x) for x in xcs]
                lb = [at(refs, x) for x in bs]
                pick_start(la, ia, xa.at[n], sems.at[1 + 4 * n])
                which = tab[where[xc_which]]
                for m, cand in enumerate(lc):
                    @pl.when((which == m + 2) if len(lc) > 1 else (which >= 0))
                    def _(cand=cand):
                        pltpu.make_async_copy(cand, xc_v.at[n], sems.at[2 + 4 * n]).start()
                if len(lc) > 1:
                    @pl.when(which < 2)
                    def _():
                        pltpu.make_async_copy(lc[0], xc_v.at[n], sems.at[2 + 4 * n]).start()
                pltpu.make_async_copy(at(refs, xr), xr_v.at[n], sems.at[3 + 4 * n]).start()
                pick_start(lb, tab[where[f"ownb{lag_s}"]], xb.at[n], sems.at[4 + 4 * n])
                waits.append((la, lc, at(refs, xr), lb))
            first.wait()
            acc[...] = base_v[...].astype(F32)
            for n, (la, lc, xr, lb) in enumerate(waits):
                pick_wait(la, xa.at[n], sems.at[1 + 4 * n])
                pick_wait(lc, xc_v.at[n], sems.at[2 + 4 * n])
                pltpu.make_async_copy(xr, xr_v.at[n], sems.at[3 + 4 * n]).wait()
                pick_wait(lb, xb.at[n], sems.at[4 + 4 * n])

                @pl.when(tab[where[f"below{steps[n][5]}"]] != 0)
                def _(n=n):
                    acc[...] -= dot(xa[n], xc_v[n])

                acc[...] -= dot(xr_v[n], xb[n])
            last = pltpu.make_async_copy(acc, out, sems.at[0])
            last.start()
            last.wait()

        n = len(steps)
        scratch = (
            [pltpu.VMEM(tile, BF16)]
            + [pltpu.VMEM((n,) + tile, BF16)] * 4
            + [pltpu.VMEM(tile, F32), pltpu.SemaphoreType.DMA((1 + 4 * n,))]
        )
        return call(
            body, kernel, table, jax.ShapeDtypeStruct(tile, F32), scratch, 2 * n * mm, f"older{s}"
        )

    def update(s, w, fresh, parts, final):
        kernel = Kernel()
        w_c = kernel.cand(w)
        xcs = [kernel.cand(x) for x in parts["xc"]]
        xrs = [kernel.cand(x) for x in parts["xr"]]
        las = [kernel.cand(*x) for x in a_moved[s]]
        bss = {
            (a, b): [kernel.cand(x[0], *x[1]) for x in all_b[s, a, b]]
            for a in range(A_CNT)
            for b in range(B_CNT)
        }
        own_xs = [kernel.cand(x) for x in solved] if final else []

        def body(tab, refs, out, w_v, acc, xa, xb, xc_v, xr_v, x_v, sems):
            flag = lambda name: tab[where[name]] != 0
            lc = [at(refs, x) for x in xcs]
            lr = [at(refs, x) for x in xrs]
            pick_start(lc, tab[where[f"xc{s}"]], xc_v, sems.at[0])
            for a in range(A_CNT):
                pick_start(lr, tab[where[f"xr{s}{a}"]], xr_v.at[a], sems.at[1 + a])
                pltpu.make_async_copy(at(refs, las[a]), xa.at[a], sems.at[1 + A_CNT + a]).start()
            base = 1 + 2 * A_CNT
            tiles_ab = [(a, b) for a in range(A_CNT) for b in range(B_CNT)]
            for n, (a, b) in enumerate(tiles_ab):
                @pl.when(flag(f"active{a}{b}"))
                def _(a=a, b=b, n=n):
                    if bss[a, b]:
                        lb = [at(refs, x) for x in bss[a, b]]
                        pick_start(lb, tab[where[f"b{s}{a}{b}"]], xb.at[n], sems.at[base + n])
                pltpu.make_async_copy(
                    at(refs, w_c).at[a, b], w_v.at[n], sems.at[base + len(tiles_ab) + n]
                ).start()
            if final:
                which = tab[where["s0"]]
                for m, x in enumerate(own_xs):
                    @pl.when((which == m) if m else ((which == 0) | (which >= FRONTS)))
                    def _(x=x):
                        pltpu.make_async_copy(at(refs, x), x_v, sems.at[base + 2 * len(tiles_ab)]).start()
            pick_wait(lc, xc_v, sems.at[0])
            for a in range(A_CNT):
                pick_wait(lr, xr_v.at[a], sems.at[1 + a])
                pltpu.make_async_copy(at(refs, las[a]), xa.at[a], sems.at[1 + A_CNT + a]).wait()
            if final:
                pltpu.make_async_copy(
                    at(refs, own_xs[0]), x_v, sems.at[base + 2 * len(tiles_ab)]
                ).wait()
            outs = []
            for n, (a, b) in enumerate(tiles_ab):
                pltpu.make_async_copy(
                    at(refs, w_c).at[a, b], w_v.at[n], sems.at[base + len(tiles_ab) + n]
                ).wait()
                acc[n] = w_v[n].astype(F32)

                @pl.when(flag(f"active{a}{b}"))
                def _(a=a, b=b, n=n):
                    if bss[a, b]:
                        lb = [at(refs, x) for x in bss[a, b]]
                        pick_wait(lb, xb.at[n], sems.at[base + n])

                        @pl.when(flag(f"rowok{s}{a}"))
                        def _():
                            acc[n] -= dot(xr_v[a], xb[n])

                    @pl.when(flag(f"col{s}{b}"))
                    def _():
                        acc[n] -= dot(xa[a], xc_v[...])

                if final:
                    @pl.when(flag(f"own{a}{b}"))
                    def _(n=n):
                        acc[n] = x_v[...].astype(F32)
                cp = pltpu.make_async_copy(
                    acc.at[n], out.at[a, b], sems.at[base + len(tiles_ab) + n]
                )
                cp.start()
                outs.append(cp)
            for cp in outs:
                cp.wait()

        count = A_CNT * B_CNT
        scratch = [
            pltpu.VMEM((count,) + tile, w.dtype),
            pltpu.VMEM((count,) + tile, F32),
            pltpu.VMEM((A_CNT,) + tile, BF16),
            pltpu.VMEM((count,) + tile, BF16),
            pltpu.VMEM(tile, BF16),
            pltpu.VMEM((A_CNT,) + tile, BF16),
            pltpu.VMEM(tile, BF16),
            pltpu.SemaphoreType.DMA((2 + 2 * A_CNT + 2 * count,)),
        ]
        return call(
            body, kernel, table, jax.ShapeDtypeStruct((A_CNT, B_CNT) + tile, F32), scratch,
            6 * mm, f"update{s}",
        )

    def column_first(s, x):
        return send(x, [(dev(r, c), dev(r - 1, c)) for k, r, c in plan.sources(s) if k > 0])

    def column_rest(s, x, p1):
        src = list(plan.sources(s))
        if not plan.pairs_of_rows:
            return [p1] + [
                send(x, [(dev(r, c), dev(r - m, c)) for k, r, c in src]) for m in range(2, R)
            ]
        p2 = send(
            x, [(dev(r, c), dev(r + 2 if r % 2 else r + 1, c)) for k, r, c in src if k > 0]
        )
        relay = p1 + p2
        p3 = send(
            relay,
            [
                (dev(r + 2, c), dev((r + 2) ^ 1, c)) if r % 2 else (dev(r - 1, c), dev((r - 1) ^ 1, c))
                for k, r, c in src
                if k > 0
            ],
        )
        return [p1, p2, p3]

    def across_columns(s, x, lag):
        return send(x, [(dev(r, c), dev(r, c + lag)) for k, r, c in plan.sources(s)])

    def ring(s, x):
        outs = [x]
        src = list(plan.sources(s))
        v = x
        for h in range(1, plan.forward + 1):
            v = send(
                v,
                [
                    (
                        dev(r, plan.ring[(plan.pos[c] + h - 1) % N]),
                        dev(r, plan.ring[(plan.pos[c] + h) % N]),
                    )
                    for k, r, c in src
                ],
            )
            outs.append(v)
        v = x
        for h in range(1, plan.backward + 1):
            v = send(
                v,
                [
                    (
                        dev(r, plan.ring[(plan.pos[c] - h + 1) % N]),
                        dev(r, plan.ring[(plan.pos[c] - h) % N]),
                    )
                    for k, r, c in src
                ],
            )
            outs.append(v)
        return outs

    a_moved[0] = [(x,) for x in a_moved[0]]
    a_moved[1] = [(upper_a, a) for a in range(A_CNT)]
    for s in (2, 3):
        a_moved[s] = [(send(upper_a[a], plan.a_pairs(s, a)),) for a in range(A_CNT)]

    solved, col_x, lag_x, rings = [], [], {}, []
    for s in range(FRONTS):
        terms = []
        for t in range(s - 1):
            xcs = col_x[t][1:] if plan.pairs_of_rows else [col_x[t][s - t - 1]]
            terms.append((a_moved[t], xcs, f"xc{t}", lag_x[t, s - t], own_b[t], t))
        base, indexed = (older(s, terms), False) if terms else (c_stack, True)
        lag1 = []
        if s:
            lag1.append((a_moved[s - 1], col_x[s - 1][0], lag_x[s - 1, 1], own_b[s - 1], s - 1))
        x = solve(s, base, indexed, lag1)
        solved.append(x)
        p1 = column_first(s, x)
        if s + 1 < FRONTS:
            lag_x[s, 1] = across_columns(s, x, 1)
        col_x.append(column_rest(s, x, p1))
        for m in range(2, FRONTS - s):
            lag_x[s, m] = across_columns(s, x, m)
        rings.append(ring(s, x))

    w = c_stack
    for s in range(FRONTS):
        parts = {"xc": [solved[s]] + col_x[s], "xr": rings[s]}
        w = update(s, w, s == 0, parts, s == FRONTS - 1)
    return jnp.transpose(w, (0, 2, 1, 3))


def solution(mesh):
    return jax.shard_map(
        shards,
        mesh=mesh,
        in_specs=(
            P(None, "row", "col"),
            P(None, "row", None, "col"),
            P(None, "row", None, "col"),
            P(None, "row", None),
            P(None, "col", None),
            P(None, "row"),
            P(None, "col"),
        ),
        out_specs=P(None, "row", None, "col"),
        check_vma=False,
    )
```

```python
import jax
import jax.numpy as jnp
import numpy as np
from jax import lax
from jax.experimental import pallas as pl
from jax.experimental.pallas import tpu as pltpu
from jax.sharding import PartitionSpec as P


FRONTS = 4
AXES = ("row", "col")
ANY = pl.BlockSpec(memory_space=pl.ANY)
SMEM = pl.BlockSpec(memory_space=pltpu.SMEM)
F32 = jnp.float32
BF16 = jnp.bfloat16


def send(block, pairs):
    return lax.ppermute(block, AXES, sorted(pairs))


class Plan:
    def __init__(self, R, N, a_count, b_count, b_rows):
        self.R, self.N = R, N
        self.a_count, self.b_count, self.b_rows = a_count, b_count, b_rows
        self.pairs_of_rows = R == 4
        half = N // 2
        self.ring = [2 * i for i in range(half)] + [2 * i + 1 for i in reversed(range(half))]
        self.pos = {c: p for p, c in enumerate(self.ring)}
        self.forward = N // 2
        self.backward = N - 1 - self.forward

    def dev(self, r, c):
        return (r % self.R) * self.N + c % self.N

    def sources(self, s):
        for k in range(self.N):
            j = k + s - 1
            if j >= 0:
                yield k, k % self.R, j % self.N

    def column_needs(self, row, k):
        return row < k

    def a_pairs(self, s, a):
        out = []
        for r in range(self.R):
            for c in range(self.N):
                if s == 0 and c == 0:
                    continue
                if r + self.R * a < (c - 1 if s == 2 else c):
                    out.append((self.dev(r, c), self.dev(r, c + s - 1)))
        return out

    def b_reads(self, r, c):
        got = set()
        for s in range(FRONTS):
            for a in range(self.a_count):
                l = r + self.R * a - 1 + s
                for b in range(self.b_count):
                    if 0 <= l < c + self.N * b:
                        got.add((l % self.R, l // self.R, b))
        return got

    def b_tiles(self):
        got = set()
        for r in range(self.R):
            for c in range(self.N):
                got |= {(a, b) for _, a, b in self.b_reads(r, c)}
        return sorted(got, key=lambda t: (t[1], -t[0]))


def pick_start(cands, which, dst, sem):
    if len(cands) == 1:
        pltpu.make_async_copy(cands[0], dst, sem).start()
        return
    for n, cand in enumerate(cands):
        @pl.when(which == n)
        def _(cand=cand):
            pltpu.make_async_copy(cand, dst, sem).start()


def pick_wait(cands, dst, sem):
    pltpu.make_async_copy(cands[0], dst, sem).wait()


def dot(x, y):
    return jnp.dot(x, y, preferred_element_type=F32)


class Later:
    value = None


class Kernel:
    def __init__(self):
        self.arrays, self.ids = [], {}

    def add(self, array):
        array = array.value if isinstance(array, Later) else array
        if id(array) not in self.ids:
            self.ids[id(array)] = len(self.arrays)
            self.arrays.append(array)
        return self.ids[id(array)]

    def cand(self, array, *index):
        return (self.add(array), index)


def at(refs, cand):
    n, index = cand
    return refs[n].at[index] if index else refs[n]


def call(body, kernel, table, out_shape, scratch, flops, aliases=None):
    n = len(kernel.arrays)

    def wrapped(table_ref, *rest):
        body(table_ref, rest[:n], rest[n], *rest[n + 1:])

    return pl.pallas_call(
        wrapped,
        out_shape=out_shape,
        in_specs=[SMEM] + [ANY] * n,
        out_specs=ANY,
        scratch_shapes=scratch,
        input_output_aliases=aliases or {},
        cost_estimate=pl.CostEstimate(flops=flops, bytes_accessed=1 << 22, transcendentals=0),
    )(table, *kernel.arrays)


def steps(upper_a, upper_b, right_side, a_bases, b_bases, a_values, b_values):
    R = lax.axis_size("row")
    N = lax.axis_size("col")
    A_CNT, B_CNT, B_ROWS = right_side.shape[0], right_side.shape[2], upper_b.shape[0]
    nb = right_side.shape[1]
    plan = Plan(R, N, A_CNT, B_CNT, B_ROWS)
    dev = plan.dev
    tile = (nb, nb)
    mm = 2 * nb**3

    columns = {}

    def column(name, fn):
        columns[name] = np.array([fn(r, c) for r in range(R) for c in range(N)], np.int32)

    def own(r, c):
        s = (c - r + 1) % R
        if s >= FRONTS:
            return None
        k = (c - s + 1)
        if k >= N:
            return None
        b = 0
        if k < 0:
            k, b = k + N, 1
        return s, k, k // R, b

    column("a0", lambda r, c: (own(r, c) or (0, 0, 0, 0))[2])
    column("b0", lambda r, c: (own(r, c) or (0, 0, 0, 0))[3])
    column("s0", lambda r, c: (own(r, c) or (FRONTS, 0, 0, 0))[0])
    for a in range(A_CNT):
        for b in range(B_CNT):
            column(f"active{a}{b}", lambda r, c: int(c + N * b > r + R * a + FRONTS - 2))
            column(
                f"own{a}{b}",
                lambda r, c: int(own(r, c) is not None and own(r, c)[2:] == (a, b)),
            )
    for s in range(FRONTS):
        for b in range(B_CNT):
            def col_valid(r, c):
                k = c - s + 1
                return int(k < N and (0 if k >= 0 else 1) == b)

            column(f"col{s}{b}", col_valid)

    for t in range(FRONTS - 1):
        column(
            f"below{t}",
            lambda r, c: int(
                own(r, c) is not None and own(r, c)[0] > t and own(r, c)[1] + own(r, c)[0] - t < N
            ),
        )

    c_stack = jnp.transpose(right_side, (0, 2, 1, 3))

    def own_of(row, col):
        front = lax.rem(col - row + 1 + R, R)
        k = col - front + 1
        b = (k < 0).astype(jnp.int32)
        return front, k + N * b, b

    a_moved = {1: [(upper_a, a) for a in range(A_CNT)]}

    def move_a(s):
        a_moved[s] = [(send(upper_a[a], plan.a_pairs(s, a)),) for a in range(A_CNT)]

    tiles = plan.b_tiles()
    b_main = 1 + max(a for a, b in tiles if b == 0)
    b_rows = 1 + max(a for a, _ in tiles)
    both = jnp.transpose(upper_b[:b_main], (2, 0, 1, 3))
    home, urgent = {}, {}
    for a, b in tiles:
        home[a, b] = (both, (b, a)) if a < b_main else None
    tall = Later()
    for a in range(b_main, b_rows):
        home[a, B_CNT - 1] = (tall, (a,))

    if plan.pairs_of_rows:
        wanted = {}
        for r in range(R):
            for c in range(N):
                o = own(r, c)
                if o is None:
                    continue
                for t in range(o[0]):
                    l, j = o[1] - 1 + t, c + N * o[3]
                    if not 0 <= l < j or (r ^ (l % R)) < 2:
                        continue
                    assert (l % R, c) not in wanted
                    wanted[l % R, c] = (r, l // R, o[3])
        row_id, col_id = lax.axis_index("row"), lax.axis_index("col")
        odd = row_id % 2
        _, dst_k, dst_b = own_of(lax.rem(row_id + 2 * odd - 1 + R, R), col_id)
        early = jnp.clip((dst_k + 1 - 2 * odd) // R, 0, b_rows - 1), dst_b
        urgent_tile = lax.dynamic_slice(
            upper_b, (early[0], 0, early[1], 0), (1, nb, 1, nb)
        ).reshape(tile)
        urgent_moved = send(
            urgent_tile, [(dev(r, c), dev(w[0], c)) for (r, c), w in wanted.items()]
        )
        urgent = {(w[0], c, r, w[1], w[2]): (urgent_moved, ()) for (r, c), w in wanted.items()}
        mates = [(dev(r, c), dev(r ^ 1, c)) for r in range(R) for c in range(N)]
        mate_both = send(both, mates)
        mate = {t: (mate_both, (t[1], t[0])) for t in tiles if t[0] < b_main}
        across, across_mate = {}, {}

        places = [(r, c) for r in range(R) for c in range(N)]

        def move_b(members, moved, passed):
            across_pairs = [
                (dev(r, c), dev(r ^ 2, c))
                for r, c in places
                if any((r, *t) in plan.b_reads(d, c) for t in members for d in (r ^ 2, r ^ 3))
            ]
            pass_pairs = [
                (dev(r, c), dev(r ^ 1, c))
                for r, c in places
                if any((r ^ 2, *t) in plan.b_reads(r ^ 1, c) for t in members)
            ]
            for t, index in members.items():
                across[t] = (moved, index)
                across_mate[t] = (passed, index)

            def go(block):
                moved.value = send(block, across_pairs)
                passed.value = send(moved.value, pass_pairs)

            return go

        for b in range(B_CNT - 1):
            members = {(a, b): (a,) for a in range(b_main)}
            move_b(members, Later(), Later())(both[b])
        members = {(a, B_CNT - 1): (a,) for a in range(b_rows)}
        go_tall = move_b(members, Later(), Later())

        def move_tall(x):
            tall.value = lax.optimization_barrier((upper_b, x))[0][:b_rows, :, B_CNT - 1]
            go_tall(tall.value)

        def b_source(r, src, t):
            return {0: home, 1: mate, 2: across, 3: across_mate}[r ^ src].get(t)
    else:
        tall.value = upper_b[:b_rows, :, B_CNT - 1]
        move_tall = lambda x: None
        shifted = {1: home}
        for s in (0, 2, 3):
            pairs = [(dev(r + s - 1, c), dev(r, c)) for r in range(R) for c in range(N)]
            moved = send(both, pairs)
            moved_tall = send(tall.value, pairs)
            shifted[s] = {
                t: (moved, (t[1], t[0])) if t[0] < b_main else (moved_tall, (t[0],)) for t in tiles
            }

        def b_source(r, src, t):
            return shifted[(src - r + 1) % R].get(t)

    def b_cands(name, s, reads):
        cands, keys, choice = [], {}, []
        for r in range(R):
            for c in range(N):
                n = 0
                ab = reads(r, c)
                if ab is not None:
                    a, b = ab
                    l = r + R * a - 1 + s
                    if 0 <= l < c + N * b:
                        cand = b_source(r, l % R, (l // R, b))
                        if name.startswith("own"):
                            cand = urgent.get((r, c, l % R, l // R, b), cand)
                        key = (id(cand[0]), cand[1])
                        if key not in keys:
                            keys[key] = len(cands)
                            cands.append(cand)
                        n = keys[key]
                choice.append(n)
        columns[name] = np.array(choice, np.int32)
        return cands

    own_b = {}
    for s in range(1, FRONTS):
        for t in range(s):
            def reads(r, c, s=s):
                o = own(r, c)
                return o[2:] if o is not None and o[0] == s else None

            own_b[s, t] = b_cands(f"ownb{s}{t}", t, reads)
    all_b = {}
    for s in range(FRONTS):
        for a in range(A_CNT):
            for b in range(B_CNT):
                def reads(r, c, a=a, b=b):
                    return (a, b) if c + N * b > r + R * a + FRONTS - 2 else None

                all_b[s, a, b] = b_cands(f"b{s}{a}{b}", s, reads)
    for s in range(FRONTS):
        for a in range(A_CNT):
            def row_pick(r, c):
                k = r + R * a
                if k + s - 1 < 0:
                    return 0
                dist = (plan.pos[c] - plan.pos[(k + s - 1) % N]) % N
                return dist if dist <= plan.forward else plan.forward + N - dist

            column(f"xr{s}{a}", row_pick)

        def col_pick(r, c):
            k = (c - s + 1) % N
            off = (k - r) % R
            if off == 0:
                return 0
            if not plan.pairs_of_rows:
                return off
            return r ^ (k % R)

        column(f"xc{s}", col_pick)
    early_hops = [0, *range(1, plan.forward // 2 + 1)]
    early_hops += [plan.forward + h for h in range(1, plan.backward // 2 + 2)]
    late_hops = [h for h in range(N) if h not in early_hops]
    for part, hops in enumerate((early_hops, late_hops)):
        for a in range(A_CNT):
            for s in range(FRONTS):
                at_dev = lambda r, c: int(columns[f"xr{s}{a}"][r * N + c])
                column(
                    f"part{part}_{a}{s}",
                    lambda r, c: int(r + R * a + s - 1 >= 0 and at_dev(r, c) in hops),
                )
    for b in range(B_CNT):
        for s in range(FRONTS):
            columns[f"col{b}_{s}"] = columns[f"col{s}{b}"]

    names = list(columns)
    where = {name: n for n, name in enumerate(names)}
    table = jnp.asarray(np.stack([columns[n] for n in names], 1))
    me = lax.axis_index("row") * N + lax.axis_index("col")
    table = lax.dynamic_slice_in_dim(table, me, 1, 0)[0]
    _, own_k, b0 = own_of(lax.axis_index("row"), lax.axis_index("col"))
    a0 = jnp.minimum(own_k // R, A_CNT - 1)
    denominators = (
        lax.dynamic_index_in_dim(a_values, a0, 0, False)[:, None]
        + lax.dynamic_index_in_dim(b_values, b0, 0, False)[None, :]
    )

    def solve(s, base, base_index, terms, before):
        kernel = Kernel()
        base_c = kernel.cand(base)
        qa_c, qb_c, d_c = kernel.cand(a_bases), kernel.cand(b_bases), kernel.cand(denominators)
        before_c = kernel.cand(before) if before is not None else None
        steps = [
            (
                [kernel.cand(*x) for x in ([(next_a,)] if (s, t) == (3, 2) else a_moved[t])],
                kernel.cand(xc),
                kernel.cand(xr),
                [kernel.cand(x[0], *x[1]) for x in own_b[s, t]],
                t,
            )
            for t, xc, xr in terms
        ]

        def body(tab, refs, out, base_v, qa, qb, den, xa, xb, xc_v, xr_v, y, acc, sems):
            ia, ib = tab[where["a0"]], tab[where["b0"]]
            mine = tab[where["s0"]] == s

            @pl.when(mine)
            def _():
                src = at(refs, base_c)
                copies = [
                    pltpu.make_async_copy(src.at[ia, ib] if base_index else src, base_v, sems.at[0]),
                    pltpu.make_async_copy(at(refs, qa_c).at[ia], qa, sems.at[1]),
                    pltpu.make_async_copy(at(refs, qb_c).at[ib], qb, sems.at[2]),
                    pltpu.make_async_copy(at(refs, d_c), den, sems.at[3]),
                ]
                copies[0].start()
                for n, (left_a, xc, xr, bs, t) in enumerate(steps):
                    pick_start([at(refs, x) for x in left_a], ia, xa.at[n], sems.at[4 + 4 * n])
                    pltpu.make_async_copy(at(refs, xc), xc_v.at[n], sems.at[5 + 4 * n]).start()
                    pltpu.make_async_copy(at(refs, xr), xr_v.at[n], sems.at[6 + 4 * n]).start()
                    pick_start(
                        [at(refs, x) for x in bs],
                        tab[where[f"ownb{s}{t}"]],
                        xb.at[n],
                        sems.at[7 + 4 * n],
                    )
                for cp in copies[1:]:
                    cp.start()
                copies[0].wait()
                if steps:
                    acc[...] = base_v[...].astype(F32)
                    for n, (left_a, xc, xr, bs, t) in enumerate(steps):
                        pick_wait([at(refs, left_a[0])], xa.at[n], sems.at[4 + 4 * n])
                        pltpu.make_async_copy(at(refs, xc), xc_v.at[n], sems.at[5 + 4 * n]).wait()

                        @pl.when(tab[where[f"below{t}"]] != 0)
                        def _(n=n):
                            acc[...] -= dot(xa[n], xc_v[n])

                        pltpu.make_async_copy(at(refs, xr), xr_v.at[n], sems.at[6 + 4 * n]).wait()
                        pick_wait([at(refs, bs[0])], xb.at[n], sems.at[7 + 4 * n])
                        acc[...] -= dot(xr_v[n], xb[n])
                    y[...] = acc[...].astype(BF16)
                else:
                    y[...] = base_v[...].astype(BF16)
                copies[1].wait()
                y[...] = lax.dot_general(
                    qa[...], y[...], (((0,), (0,)), ((), ())), preferred_element_type=F32
                ).astype(BF16)
                copies[2].wait()
                copies[3].wait()
                y[...] = (dot(y[...], qb[...]) / den[...]).astype(BF16)
                y[...] = dot(qa[...], y[...]).astype(BF16)
                y[...] = lax.dot_general(
                    y[...], qb[...], (((1,), (1,)), ((), ())), preferred_element_type=F32
                ).astype(BF16)
                last = pltpu.make_async_copy(y, out, sems.at[0])
                last.start()
                last.wait()

            @pl.when(jnp.logical_not(mine))
            def _():
                if before_c is not None:
                    get = pltpu.make_async_copy(at(refs, before_c), y, sems.at[0])
                    get.start()
                    get.wait()
                else:
                    y[...] = jnp.zeros_like(y)
                last = pltpu.make_async_copy(y, out, sems.at[0])
                last.start()
                last.wait()

        m = max(1, len(steps))
        scratch = [
            pltpu.VMEM(tile, base.dtype),
            pltpu.VMEM(tile, BF16),
            pltpu.VMEM(tile, BF16),
            pltpu.VMEM(tile, F32),
        ] + [pltpu.VMEM((m,) + tile, BF16)] * 4
        scratch += [pltpu.VMEM(tile, BF16), pltpu.VMEM(tile, F32)]
        scratch += [pltpu.SemaphoreType.DMA((4 + 4 * m,))]
        return call(
            body, kernel, table, jax.ShapeDtypeStruct(tile, BF16), scratch,
            (4 + 2 * len(steps)) * mm,
        )

    def older(s, terms):
        kernel = Kernel()
        base_c = kernel.cand(c_stack)
        steps = [
            (
                [kernel.cand(*x) for x in a_moved[t]],
                kernel.cand(xc),
                kernel.cand(xr),
                [kernel.cand(x[0], *x[1]) for x in own_b[s, t]],
                t,
            )
            for t, xc, xr in terms
        ]

        def body(tab, refs, out, base_v, xa, xb, xc_v, xr_v, acc, sems):
            ia, ib = tab[where["a0"]], tab[where["b0"]]

            @pl.when(tab[where["s0"]] == s)
            def _():
                first = pltpu.make_async_copy(at(refs, base_c).at[ia, ib], base_v, sems.at[0])
                first.start()
                for n, (left_a, xc, xr, bs, t) in enumerate(steps):
                    pick_start([at(refs, x) for x in left_a], ia, xa.at[n], sems.at[1 + 4 * n])
                    pltpu.make_async_copy(at(refs, xc), xc_v.at[n], sems.at[2 + 4 * n]).start()
                    pltpu.make_async_copy(at(refs, xr), xr_v.at[n], sems.at[3 + 4 * n]).start()
                    pick_start(
                        [at(refs, x) for x in bs],
                        tab[where[f"ownb{s}{t}"]],
                        xb.at[n],
                        sems.at[4 + 4 * n],
                    )
                first.wait()
                acc[...] = base_v[...].astype(F32)
                for n, (left_a, xc, xr, bs, t) in enumerate(steps):
                    pick_wait([at(refs, left_a[0])], xa.at[n], sems.at[1 + 4 * n])
                    pltpu.make_async_copy(at(refs, xc), xc_v.at[n], sems.at[2 + 4 * n]).wait()
                    pltpu.make_async_copy(at(refs, xr), xr_v.at[n], sems.at[3 + 4 * n]).wait()
                    pick_wait([at(refs, bs[0])], xb.at[n], sems.at[4 + 4 * n])

                    @pl.when(tab[where[f"below{t}"]] != 0)
                    def _(n=n):
                        acc[...] -= dot(xa[n], xc_v[n])

                    acc[...] -= dot(xr_v[n], xb[n])
                last = pltpu.make_async_copy(acc, out, sems.at[0])
                last.start()
                last.wait()

        n = len(steps)
        scratch = (
            [pltpu.VMEM(tile, BF16)]
            + [pltpu.VMEM((n,) + tile, BF16)] * 4
            + [pltpu.VMEM(tile, F32), pltpu.SemaphoreType.DMA((1 + 4 * n,))]
        )
        return call(body, kernel, table, jax.ShapeDtypeStruct(tile, F32), scratch, 2 * n * mm)

    def update(part, w, hops, rows_x, columns_x, final_x):
        kernel = Kernel()
        w_c = kernel.cand(w)
        fronts = range(FRONTS)
        tiles_ab = [(a, b) for a in range(A_CNT) for b in range(B_CNT)]
        count = len(tiles_ab)
        xrs = {h: kernel.cand(rows_x[h]) for h in hops}
        xcs = [kernel.cand(x) for x in columns_x]
        las = {s: [kernel.cand(*x) for x in a_moved[s]] for s in fronts} if columns_x else None
        bss = {
            (s, a, b): [kernel.cand(x[0], *x[1]) for x in all_b[s, a, b]]
            for s in fronts
            for a, b in tiles_ab
        }
        final_c = kernel.cand(final_x) if final_x is not None else None
        lanes = 128
        chunks = nb // lanes

        def body(tab, refs, out, w_v, acc, xa, xb, xc_v, xr_v, x_v, out_v, sem_r, sem_b, sem_c, sem_w):
            flag = lambda name: tab[where[name]] != 0
            for s in fronts:
                for a in range(A_CNT):
                    @pl.when(flag(f"part{part}_{a}{s}"))
                    def _(s=s, a=a):
                        which = tab[where[f"xr{s}{a}"]]
                        for h in hops:
                            @pl.when(which == h)
                            def _(h=h):
                                pltpu.make_async_copy(
                                    at(refs, xrs[h]), xr_v.at[a, s], sem_r.at[a, s]
                                ).start()
                        for b in range(B_CNT):
                            if bss[s, a, b]:
                                @pl.when(flag(f"active{a}{b}"))
                                def _(b=b):
                                    lb = [at(refs, x) for x in bss[s, a, b]]
                                    n = a * B_CNT + b
                                    pick_start(
                                        lb, tab[where[f"b{s}{a}{b}"]], xb.at[n, s], sem_b.at[n, s]
                                    )
            for n, (a, b) in enumerate(tiles_ab):
                pltpu.make_async_copy(at(refs, w_c).at[a, b], w_v.at[n], sem_w.at[n]).start()
            if final_c is not None:
                pltpu.make_async_copy(at(refs, final_c), x_v, sem_w.at[count]).start()
            if columns_x:
                lc = [at(refs, x) for x in xcs]
                for s in fronts:
                    pick_start(lc, tab[where[f"xc{s}"]], xc_v.at[s], sem_c.at[s])
                    for a in range(A_CNT):
                        pltpu.make_async_copy(at(refs, las[s][a]), xa.at[a, s], sem_c.at[s]).start()
            some = at(refs, kernel.cand(rows_x[hops[0]]))
            for n in range(count):
                pltpu.make_async_copy(at(refs, w_c).at[0, 0], w_v.at[n], sem_w.at[n]).wait()
                acc[n] = w_v[n].astype(F32)
            for a in range(A_CNT):
                def row_step(s, carry, a=a):
                    @pl.when(tab[where[f"part{part}_{a}0"] + s] != 0)
                    def _():
                        pltpu.make_async_copy(some, xr_v.at[a, s], sem_r.at[a, s]).wait()
                        for b in range(B_CNT):
                            n = a * B_CNT + b

                            @pl.when(flag(f"active{a}{b}"))
                            def _(n=n):
                                pltpu.make_async_copy(some, xb.at[n, s], sem_b.at[n, s]).wait()
                                acc[n] -= dot(xr_v[a, s], xb[n, s])

                    return carry

                lax.fori_loop(0, FRONTS, row_step, 0)
            if columns_x:
                def column_step(s, carry):
                    for _ in range(1 + A_CNT):
                        pltpu.make_async_copy(some, xc_v.at[s], sem_c.at[s]).wait()
                    for b in range(B_CNT):
                        @pl.when(tab[where[f"col{b}_0"] + s] != 0)
                        def _(b=b):
                            for a in range(A_CNT):
                                n = a * B_CNT + b

                                @pl.when(flag(f"active{a}{b}"))
                                def _(a=a, n=n):
                                    acc[n] -= dot(xa[a, s], xc_v[s])

                    return carry

                lax.fori_loop(0, FRONTS, column_step, 0)
            if final_c is None:
                outs = [
                    pltpu.make_async_copy(acc.at[n], out.at[a, b], sem_w.at[n])
                    for n, (a, b) in enumerate(tiles_ab)
                ]
                for cp in outs:
                    cp.start()
                for cp in outs:
                    cp.wait()
                return
            pltpu.make_async_copy(at(refs, final_c), x_v, sem_w.at[count]).wait()
            outs = []
            for a in range(A_CNT):
                for b in range(B_CNT):
                    n = a * B_CNT + b

                    @pl.when(flag(f"own{a}{b}"))
                    def _(n=n):
                        acc[n] = x_v[...].astype(F32)

                    for q in range(chunks):
                        out_v[a, :, q * B_CNT + b, :] = acc[n, :, q * lanes : (q + 1) * lanes]
                cp = pltpu.make_async_copy(out_v.at[a], out.at[a], sem_w.at[a])
                cp.start()
                outs.append(cp)
            for cp in outs:
                cp.wait()

        wide = final_x is not None
        out_tile = (A_CNT, nb, chunks * B_CNT, lanes)
        scratch = [
            pltpu.VMEM((count,) + tile, w.dtype),
            pltpu.VMEM((count,) + tile, F32),
            pltpu.VMEM((A_CNT, FRONTS) + tile if columns_x else (1, 1, 8, 128), BF16),
            pltpu.VMEM((count, FRONTS) + tile, BF16),
            pltpu.VMEM((FRONTS,) + tile, BF16),
            pltpu.VMEM((A_CNT, FRONTS) + tile, BF16),
            pltpu.VMEM(tile, BF16),
            pltpu.VMEM(out_tile if wide else (1, 8, 8, 128), F32),
            pltpu.SemaphoreType.DMA((A_CNT, FRONTS)),
            pltpu.SemaphoreType.DMA((count, FRONTS)),
            pltpu.SemaphoreType.DMA((FRONTS,)),
            pltpu.SemaphoreType.DMA((count + 1,)),
        ]
        shape = out_tile if wide else (A_CNT, B_CNT) + tile
        return call(body, kernel, table, jax.ShapeDtypeStruct(shape, F32), scratch, 12 * mm)

    def lagged(x, which):
        down, right = [], []
        for s, lag in which:
            for k, r, c in plan.sources(s):
                if k - lag >= 0:
                    down.append((dev(r, c), dev(r - lag, c)))
                right.append((dev(r, c), dev(r, c + lag)))
        return send(x, down), send(x, right)

    def ring(fronts, x):
        outs = [x]
        src = [p for s in fronts for p in plan.sources(s)]
        for sign, hops in ((1, plan.forward), (-1, plan.backward)):
            v = x
            for h in range(hops):
                at_hop = lambda c, h: plan.ring[(plan.pos[c] + sign * h) % N]
                v = send(v, [(dev(r, at_hop(c, h)), dev(r, at_hop(c, h + 1))) for k, r, c in src])
                outs.append(v)
        return outs

    def column_all(x):
        if not plan.pairs_of_rows:
            return [x] + [
                send(x, [(dev(r + m, c), dev(r, c)) for r in range(R) for c in range(N)])
                for m in range(1, R)
            ]
        places = [(r, c) for r in range(R) for c in range(N)]
        swap = lambda v, m: send(v, [(dev(r, c), dev(r ^ m, c)) for r, c in places])
        other = swap(x, 2)
        return [x, swap(x, 1), other, swap(other, 1)]

    move_a(0)
    move_a(3)
    next_a = send(
        lax.dynamic_index_in_dim(upper_a, a0, 0, False),
        [(dev(r, c), dev(r, c + 1)) for k, r, c in plan.sources(2) if k + 1 < N],
    )
    x0 = solve(0, c_stack, True, [], None)
    col_a, row_a = lagged(x0, [(0, 1)])
    col_e, row_e = lagged(x0, [(0, 2)])
    x1 = solve(1, c_stack, True, [(0, col_a, row_a)], x0)
    col_b, row_b = lagged(x1, [(1, 1), (0, 3)])
    col_c, row_c = lagged(x1, [(1, 2)])
    move_tall(x1)
    x2 = solve(2, c_stack, True, [(0, col_e, row_e), (1, col_b, row_b)], x1)
    col_d, row_d = lagged(x2, [(2, 1)])
    move_a(2)
    base = older(3, [(0, col_b, row_b), (1, col_c, row_c)])
    x3 = solve(3, base, False, [(2, col_d, row_d)], x2)
    rows_x = ring(range(FRONTS), x3)
    w = update(0, c_stack, early_hops, rows_x, column_all(x3), None)
    w = update(1, w, late_hops, rows_x, [], x3)
    w = w.reshape(A_CNT, nb, w.shape[2] // B_CNT, B_CNT, w.shape[3])
    return jnp.transpose(w, (0, 1, 3, 2, 4)).reshape(right_side.shape)


def solution(mesh):
    return jax.shard_map(
        steps,
        mesh=mesh,
        in_specs=(
            P(None, "row", "col"),
            P(None, "row", None, "col"),
            P(None, "row", None, "col"),
            P(None, "row", None),
            P(None, "col", None),
            P(None, "row"),
            P(None, "col"),
        ),
        out_specs=P(None, "row", None, "col"),
        check_vma=False,
    )
```

```python
import jax
import jax.numpy as jnp
import numpy as np
from jax import lax
from jax.experimental import pallas as pl
from jax.experimental.pallas import tpu as pltpu
from jax.sharding import PartitionSpec as P


FRONTS = 4
AXES = ("row", "col")
ANY = pl.BlockSpec(memory_space=pl.ANY)
SMEM = pl.BlockSpec(memory_space=pltpu.SMEM)
F32 = jnp.float32
BF16 = jnp.bfloat16


def send(block, pairs):
    return lax.ppermute(block, AXES, sorted(pairs))


class Plan:
    def __init__(self, R, N, a_count, b_count, b_rows):
        self.R, self.N = R, N
        self.a_count, self.b_count, self.b_rows = a_count, b_count, b_rows
        self.pairs_of_rows = R == 4
        half = N // 2
        self.ring = [2 * i for i in range(half)] + [2 * i + 1 for i in reversed(range(half))]
        self.pos = {c: p for p, c in enumerate(self.ring)}
        self.forward = N // 2
        self.backward = N - 1 - self.forward

    def dev(self, r, c):
        return (r % self.R) * self.N + c % self.N

    def sources(self, s):
        for k in range(self.N):
            j = k + s - 1
            if j >= 0:
                yield k, k % self.R, j % self.N

    def column_needs(self, row, k):
        return row < k

    def a_pairs(self, s, a):
        out = []
        for r in range(self.R):
            for c in range(self.N):
                if s == 0 and c == 0:
                    continue
                if r + self.R * a < (c - 1 if s == 2 else c):
                    out.append((self.dev(r, c), self.dev(r, c + s - 1)))
        return out

    def b_reads(self, r, c):
        got = set()
        for s in range(FRONTS):
            for a in range(self.a_count):
                l = r + self.R * a - 1 + s
                for b in range(self.b_count):
                    if 0 <= l < c + self.N * b:
                        got.add((l % self.R, l // self.R, b))
        return got

    def b_tiles(self):
        got = set()
        for r in range(self.R):
            for c in range(self.N):
                got |= {(a, b) for _, a, b in self.b_reads(r, c)}
        return sorted(got, key=lambda t: (t[1], -t[0]))


def pick_start(cands, which, dst, sem):
    if len(cands) == 1:
        pltpu.make_async_copy(cands[0], dst, sem).start()
        return
    for n, cand in enumerate(cands):
        @pl.when(which == n)
        def _(cand=cand):
            pltpu.make_async_copy(cand, dst, sem).start()


def pick_wait(cands, dst, sem):
    pltpu.make_async_copy(cands[0], dst, sem).wait()


def dot(x, y):
    return jnp.dot(x, y, preferred_element_type=F32)


class Later:
    value = None


class Kernel:
    def __init__(self):
        self.arrays, self.ids = [], {}

    def add(self, array):
        array = array.value if isinstance(array, Later) else array
        if id(array) not in self.ids:
            self.ids[id(array)] = len(self.arrays)
            self.arrays.append(array)
        return self.ids[id(array)]

    def cand(self, array, *index):
        return (self.add(array), index)


def at(refs, cand):
    n, index = cand
    return refs[n].at[index] if index else refs[n]


def call(body, kernel, table, out_shape, scratch, flops, aliases=None):
    n = len(kernel.arrays)

    def wrapped(table_ref, *rest):
        body(table_ref, rest[:n], rest[n], *rest[n + 1:])

    return pl.pallas_call(
        wrapped,
        out_shape=out_shape,
        in_specs=[SMEM] + [ANY] * n,
        out_specs=ANY,
        scratch_shapes=scratch,
        input_output_aliases=aliases or {},
        cost_estimate=pl.CostEstimate(flops=flops, bytes_accessed=1 << 22, transcendentals=0),
    )(table, *kernel.arrays)


def steps(upper_a, upper_b, right_side, a_bases, b_bases, a_values, b_values):
    R = lax.axis_size("row")
    N = lax.axis_size("col")
    A_CNT, B_CNT, B_ROWS = right_side.shape[0], right_side.shape[2], upper_b.shape[0]
    nb = right_side.shape[1]
    plan = Plan(R, N, A_CNT, B_CNT, B_ROWS)
    dev = plan.dev
    tile = (nb, nb)
    mm = 2 * nb**3

    columns = {}

    def column(name, fn):
        columns[name] = np.array([fn(r, c) for r in range(R) for c in range(N)], np.int32)

    def own(r, c):
        s = (c - r + 1) % R
        if s >= FRONTS:
            return None
        k = (c - s + 1)
        if k >= N:
            return None
        b = 0
        if k < 0:
            k, b = k + N, 1
        return s, k, k // R, b

    column("a0", lambda r, c: (own(r, c) or (0, 0, 0, 0))[2])
    column("b0", lambda r, c: (own(r, c) or (0, 0, 0, 0))[3])
    column("s0", lambda r, c: (own(r, c) or (FRONTS, 0, 0, 0))[0])
    for a in range(A_CNT):
        for b in range(B_CNT):
            column(f"active{a}{b}", lambda r, c: int(c + N * b > r + R * a + FRONTS - 2))
            column(
                f"own{a}{b}",
                lambda r, c: int(own(r, c) is not None and own(r, c)[2:] == (a, b)),
            )
    for s in range(FRONTS):
        for b in range(B_CNT):
            def col_valid(r, c):
                k = c - s + 1
                return int(k < N and (0 if k >= 0 else 1) == b)

            column(f"col{s}{b}", col_valid)

    for t in range(FRONTS - 1):
        column(
            f"below{t}",
            lambda r, c: int(
                own(r, c) is not None and own(r, c)[0] > t and own(r, c)[1] + own(r, c)[0] - t < N
            ),
        )

    c_stack = jnp.transpose(right_side, (0, 2, 1, 3))

    def own_of(row, col):
        front = lax.rem(col - row + 1 + R, R)
        k = col - front + 1
        b = (k < 0).astype(jnp.int32)
        return front, k + N * b, b

    a_moved = {1: [(upper_a, a) for a in range(A_CNT)]}

    def move_a(s):
        a_moved[s] = [(send(upper_a[a], plan.a_pairs(s, a)),) for a in range(A_CNT)]

    tiles = plan.b_tiles()
    b_main = 1 + max(a for a, b in tiles if b == 0)
    b_rows = 1 + max(a for a, _ in tiles)
    both = jnp.transpose(upper_b[:b_main], (2, 0, 1, 3))
    home, urgent = {}, {}
    for a, b in tiles:
        home[a, b] = (both, (b, a)) if a < b_main else None
    tall = Later()
    for a in range(b_main, b_rows):
        home[a, B_CNT - 1] = (tall, (a,))

    if plan.pairs_of_rows:
        wanted = {}
        for r in range(R):
            for c in range(N):
                o = own(r, c)
                if o is None:
                    continue
                for t in range(o[0]):
                    l, j = o[1] - 1 + t, c + N * o[3]
                    if not 0 <= l < j or (r ^ (l % R)) < 2:
                        continue
                    assert (l % R, c) not in wanted
                    wanted[l % R, c] = (r, l // R, o[3])
        row_id, col_id = lax.axis_index("row"), lax.axis_index("col")
        odd = row_id % 2
        _, dst_k, dst_b = own_of(lax.rem(row_id + 2 * odd - 1 + R, R), col_id)
        early = jnp.clip((dst_k + 1 - 2 * odd) // R, 0, b_rows - 1), dst_b
        urgent_tile = lax.dynamic_slice(
            upper_b, (early[0], 0, early[1], 0), (1, nb, 1, nb)
        ).reshape(tile)
        urgent_moved = send(
            urgent_tile, [(dev(r, c), dev(w[0], c)) for (r, c), w in wanted.items()]
        )
        urgent = {(w[0], c, r, w[1], w[2]): (urgent_moved, ()) for (r, c), w in wanted.items()}
        mates = [(dev(r, c), dev(r ^ 1, c)) for r in range(R) for c in range(N)]
        mate_both = send(both, mates)
        mate = {t: (mate_both, (t[1], t[0])) for t in tiles if t[0] < b_main}
        across, across_mate = {}, {}

        places = [(r, c) for r in range(R) for c in range(N)]

        def move_b(members, moved, passed):
            across_pairs = [
                (dev(r, c), dev(r ^ 2, c))
                for r, c in places
                if any((r, *t) in plan.b_reads(d, c) for t in members for d in (r ^ 2, r ^ 3))
            ]
            pass_pairs = [
                (dev(r, c), dev(r ^ 1, c))
                for r, c in places
                if any((r ^ 2, *t) in plan.b_reads(r ^ 1, c) for t in members)
            ]
            for t, index in members.items():
                across[t] = (moved, index)
                across_mate[t] = (passed, index)

            def go(block):
                moved.value = send(block, across_pairs)
                passed.value = send(moved.value, pass_pairs)

            return go

        for b in range(B_CNT - 1):
            members = {(a, b): (a,) for a in range(b_main)}
            move_b(members, Later(), Later())(both[b])
        members = {(a, B_CNT - 1): (a,) for a in range(b_rows)}
        go_tall = move_b(members, Later(), Later())

        def move_tall(x):
            tall.value = lax.optimization_barrier((upper_b, x))[0][:b_rows, :, B_CNT - 1]
            go_tall(tall.value)

        def b_source(r, src, t):
            return {0: home, 1: mate, 2: across, 3: across_mate}[r ^ src].get(t)
    else:
        tall.value = upper_b[:b_rows, :, B_CNT - 1]
        move_tall = lambda x: None
        shifted = {1: home}
        for s in (0, 2, 3):
            pairs = [(dev(r + s - 1, c), dev(r, c)) for r in range(R) for c in range(N)]
            moved = send(both, pairs)
            moved_tall = send(tall.value, pairs)
            shifted[s] = {
                t: (moved, (t[1], t[0])) if t[0] < b_main else (moved_tall, (t[0],)) for t in tiles
            }

        def b_source(r, src, t):
            return shifted[(src - r + 1) % R].get(t)

    def b_cands(name, s, reads):
        cands, keys, choice = [], {}, []
        for r in range(R):
            for c in range(N):
                n = 0
                ab = reads(r, c)
                if ab is not None:
                    a, b = ab
                    l = r + R * a - 1 + s
                    if 0 <= l < c + N * b:
                        cand = b_source(r, l % R, (l // R, b))
                        if name.startswith("own"):
                            cand = urgent.get((r, c, l % R, l // R, b), cand)
                        key = (id(cand[0]), cand[1])
                        if key not in keys:
                            keys[key] = len(cands)
                            cands.append(cand)
                        n = keys[key]
                choice.append(n)
        columns[name] = np.array(choice, np.int32)
        return cands

    own_b = {}
    for s in range(1, FRONTS):
        for t in range(s):
            def reads(r, c, s=s):
                o = own(r, c)
                return o[2:] if o is not None and o[0] == s else None

            own_b[s, t] = b_cands(f"ownb{s}{t}", t, reads)
    all_b = {}
    for s in range(FRONTS):
        for a in range(A_CNT):
            for b in range(B_CNT):
                def reads(r, c, a=a, b=b):
                    return (a, b) if c + N * b > r + R * a + FRONTS - 2 else None

                all_b[s, a, b] = b_cands(f"b{s}{a}{b}", s, reads)
    for s in range(FRONTS):
        for a in range(A_CNT):
            def row_pick(r, c):
                k = r + R * a
                if k + s - 1 < 0:
                    return 0
                dist = (plan.pos[c] - plan.pos[(k + s - 1) % N]) % N
                return dist if dist <= plan.forward else plan.forward + N - dist

            column(f"xr{s}{a}", row_pick)

        def col_pick(r, c):
            k = (c - s + 1) % N
            off = (k - r) % R
            if off == 0:
                return 0
            if not plan.pairs_of_rows:
                return off
            return r ^ (k % R)

        column(f"xc{s}", col_pick)
    early_hops = [0, *range(1, plan.forward // 2 + 1)]
    early_hops += [plan.forward + h for h in range(1, plan.backward // 2 + 2)]
    late_hops = [h for h in range(N) if h not in early_hops]
    for part, hops in enumerate((early_hops, late_hops)):
        for a in range(A_CNT):
            for s in range(FRONTS):
                at_dev = lambda r, c: int(columns[f"xr{s}{a}"][r * N + c])
                column(
                    f"part{part}_{a}{s}",
                    lambda r, c: int(r + R * a + s - 1 >= 0 and at_dev(r, c) in hops),
                )
    for b in range(B_CNT):
        for s in range(FRONTS):
            columns[f"col{b}_{s}"] = columns[f"col{s}{b}"]

    names = list(columns)
    where = {name: n for n, name in enumerate(names)}
    table = jnp.asarray(np.stack([columns[n] for n in names], 1))
    me = lax.axis_index("row") * N + lax.axis_index("col")
    table = lax.dynamic_slice_in_dim(table, me, 1, 0)[0]
    _, own_k, b0 = own_of(lax.axis_index("row"), lax.axis_index("col"))
    a0 = jnp.minimum(own_k // R, A_CNT - 1)
    denominators = (
        lax.dynamic_index_in_dim(a_values, a0, 0, False)[:, None]
        + lax.dynamic_index_in_dim(b_values, b0, 0, False)[None, :]
    )

    def solve(s, base, base_index, terms, before):
        kernel = Kernel()
        base_c = kernel.cand(base)
        qa_c, qb_c, d_c = kernel.cand(a_bases), kernel.cand(b_bases), kernel.cand(denominators)
        before_c = kernel.cand(before) if before is not None else None
        steps = [
            (
                [kernel.cand(*x) for x in ([(next_a,)] if (s, t) == (3, 2) else a_moved[t])],
                kernel.cand(xc),
                kernel.cand(xr),
                [kernel.cand(x[0], *x[1]) for x in own_b[s, t]],
                t,
            )
            for t, xc, xr in terms
        ]

        def body(tab, refs, out, base_v, qa, qb, den, xa, xb, xc_v, xr_v, y, acc, sems):
            ia, ib = tab[where["a0"]], tab[where["b0"]]
            mine = tab[where["s0"]] == s

            @pl.when(mine)
            def _():
                src = at(refs, base_c)
                copies = [
                    pltpu.make_async_copy(src.at[ia, ib] if base_index else src, base_v, sems.at[0]),
                    pltpu.make_async_copy(at(refs, qa_c).at[ia], qa, sems.at[1]),
                    pltpu.make_async_copy(at(refs, qb_c).at[ib], qb, sems.at[2]),
                    pltpu.make_async_copy(at(refs, d_c), den, sems.at[3]),
                ]
                copies[0].start()
                for n, (left_a, xc, xr, bs, t) in enumerate(steps):
                    pick_start([at(refs, x) for x in left_a], ia, xa.at[n], sems.at[4 + 4 * n])
                    pltpu.make_async_copy(at(refs, xc), xc_v.at[n], sems.at[5 + 4 * n]).start()
                    pltpu.make_async_copy(at(refs, xr), xr_v.at[n], sems.at[6 + 4 * n]).start()
                    pick_start(
                        [at(refs, x) for x in bs],
                        tab[where[f"ownb{s}{t}"]],
                        xb.at[n],
                        sems.at[7 + 4 * n],
                    )
                for cp in copies[1:]:
                    cp.start()
                copies[0].wait()
                if steps:
                    acc[...] = base_v[...].astype(F32)
                    for n, (left_a, xc, xr, bs, t) in enumerate(steps):
                        pick_wait([at(refs, left_a[0])], xa.at[n], sems.at[4 + 4 * n])
                        pltpu.make_async_copy(at(refs, xc), xc_v.at[n], sems.at[5 + 4 * n]).wait()

                        @pl.when(tab[where[f"below{t}"]] != 0)
                        def _(n=n):
                            acc[...] -= dot(xa[n], xc_v[n])

                        pltpu.make_async_copy(at(refs, xr), xr_v.at[n], sems.at[6 + 4 * n]).wait()
                        pick_wait([at(refs, bs[0])], xb.at[n], sems.at[7 + 4 * n])
                        acc[...] -= dot(xr_v[n], xb[n])
                    y[...] = acc[...].astype(BF16)
                else:
                    y[...] = base_v[...].astype(BF16)
                copies[1].wait()
                y[...] = lax.dot_general(
                    qa[...], y[...], (((0,), (0,)), ((), ())), preferred_element_type=F32
                ).astype(BF16)
                copies[2].wait()
                copies[3].wait()
                y[...] = (dot(y[...], qb[...]) / den[...]).astype(BF16)
                y[...] = dot(qa[...], y[...]).astype(BF16)
                y[...] = lax.dot_general(
                    y[...], qb[...], (((1,), (1,)), ((), ())), preferred_element_type=F32
                ).astype(BF16)
                last = pltpu.make_async_copy(y, out, sems.at[0])
                last.start()
                last.wait()

            @pl.when(jnp.logical_not(mine))
            def _():
                if before_c is not None:
                    get = pltpu.make_async_copy(at(refs, before_c), y, sems.at[0])
                    get.start()
                    get.wait()
                else:
                    y[...] = jnp.zeros_like(y)
                last = pltpu.make_async_copy(y, out, sems.at[0])
                last.start()
                last.wait()

        m = max(1, len(steps))
        scratch = [
            pltpu.VMEM(tile, base.dtype),
            pltpu.VMEM(tile, BF16),
            pltpu.VMEM(tile, BF16),
            pltpu.VMEM(tile, F32),
        ] + [pltpu.VMEM((m,) + tile, BF16)] * 4
        scratch += [pltpu.VMEM(tile, BF16), pltpu.VMEM(tile, F32)]
        scratch += [pltpu.SemaphoreType.DMA((4 + 4 * m,))]
        return call(
            body, kernel, table, jax.ShapeDtypeStruct(tile, BF16), scratch,
            (4 + 2 * len(steps)) * mm,
        )

    def older(s, terms):
        kernel = Kernel()
        base_c = kernel.cand(c_stack)
        steps = [
            (
                [kernel.cand(*x) for x in a_moved[t]],
                kernel.cand(xc),
                kernel.cand(xr),
                [kernel.cand(x[0], *x[1]) for x in own_b[s, t]],
                t,
            )
            for t, xc, xr in terms
        ]

        def body(tab, refs, out, base_v, xa, xb, xc_v, xr_v, acc, sems):
            ia, ib = tab[where["a0"]], tab[where["b0"]]

            @pl.when(tab[where["s0"]] == s)
            def _():
                first = pltpu.make_async_copy(at(refs, base_c).at[ia, ib], base_v, sems.at[0])
                first.start()
                for n, (left_a, xc, xr, bs, t) in enumerate(steps):
                    pick_start([at(refs, x) for x in left_a], ia, xa.at[n], sems.at[1 + 4 * n])
                    pltpu.make_async_copy(at(refs, xc), xc_v.at[n], sems.at[2 + 4 * n]).start()
                    pltpu.make_async_copy(at(refs, xr), xr_v.at[n], sems.at[3 + 4 * n]).start()
                    pick_start(
                        [at(refs, x) for x in bs],
                        tab[where[f"ownb{s}{t}"]],
                        xb.at[n],
                        sems.at[4 + 4 * n],
                    )
                first.wait()
                acc[...] = base_v[...].astype(F32)
                for n, (left_a, xc, xr, bs, t) in enumerate(steps):
                    pick_wait([at(refs, left_a[0])], xa.at[n], sems.at[1 + 4 * n])
                    pltpu.make_async_copy(at(refs, xc), xc_v.at[n], sems.at[2 + 4 * n]).wait()
                    pltpu.make_async_copy(at(refs, xr), xr_v.at[n], sems.at[3 + 4 * n]).wait()
                    pick_wait([at(refs, bs[0])], xb.at[n], sems.at[4 + 4 * n])

                    @pl.when(tab[where[f"below{t}"]] != 0)
                    def _(n=n):
                        acc[...] -= dot(xa[n], xc_v[n])

                    acc[...] -= dot(xr_v[n], xb[n])
                last = pltpu.make_async_copy(acc, out, sems.at[0])
                last.start()
                last.wait()

        n = len(steps)
        scratch = (
            [pltpu.VMEM(tile, BF16)]
            + [pltpu.VMEM((n,) + tile, BF16)] * 4
            + [pltpu.VMEM(tile, F32), pltpu.SemaphoreType.DMA((1 + 4 * n,))]
        )
        return call(body, kernel, table, jax.ShapeDtypeStruct(tile, F32), scratch, 2 * n * mm)

    def update(part, w, hops, rows_x, columns_x, final_x):
        kernel = Kernel()
        w_c = kernel.cand(w)
        fronts = range(FRONTS)
        tiles_ab = [(a, b) for a in range(A_CNT) for b in range(B_CNT)]
        count = len(tiles_ab)
        xrs = {h: kernel.cand(rows_x[h]) for h in hops}
        xcs = [kernel.cand(x) for x in columns_x]
        las = {s: [kernel.cand(*x) for x in a_moved[s]] for s in fronts} if columns_x else None
        bss = {
            (s, a, b): [kernel.cand(x[0], *x[1]) for x in all_b[s, a, b]]
            for s in fronts
            for a, b in tiles_ab
        }
        final_c = kernel.cand(final_x) if final_x is not None else None
        lanes = 128
        chunks = nb // lanes

        def body(tab, refs, out, w_v, acc, xa, xb, xc_v, xr_v, x_v, out_v, sem_r, sem_b, sem_c, sem_w):
            flag = lambda name: tab[where[name]] != 0
            for s in fronts:
                for a in range(A_CNT):
                    @pl.when(flag(f"part{part}_{a}{s}"))
                    def _(s=s, a=a):
                        which = tab[where[f"xr{s}{a}"]]
                        for h in hops:
                            @pl.when(which == h)
                            def _(h=h):
                                pltpu.make_async_copy(
                                    at(refs, xrs[h]), xr_v.at[a, s], sem_r.at[a, s]
                                ).start()
                        for b in range(B_CNT):
                            if bss[s, a, b]:
                                @pl.when(flag(f"active{a}{b}"))
                                def _(b=b):
                                    lb = [at(refs, x) for x in bss[s, a, b]]
                                    n = a * B_CNT + b
                                    pick_start(
                                        lb, tab[where[f"b{s}{a}{b}"]], xb.at[n, s], sem_b.at[n, s]
                                    )
            for n, (a, b) in enumerate(tiles_ab):
                pltpu.make_async_copy(at(refs, w_c).at[a, b], w_v.at[n], sem_w.at[n]).start()
            if final_c is not None:
                pltpu.make_async_copy(at(refs, final_c), x_v, sem_w.at[count]).start()
            if columns_x:
                lc = [at(refs, x) for x in xcs]
                for s in fronts:
                    pick_start(lc, tab[where[f"xc{s}"]], xc_v.at[s], sem_c.at[s])
                    for a in range(A_CNT):
                        pltpu.make_async_copy(at(refs, las[s][a]), xa.at[a, s], sem_c.at[s]).start()
            some = at(refs, kernel.cand(rows_x[hops[0]]))
            for n in range(count):
                pltpu.make_async_copy(at(refs, w_c).at[0, 0], w_v.at[n], sem_w.at[n]).wait()
                acc[n] = w_v[n].astype(F32)
            for a in range(A_CNT):
                def row_step(s, carry, a=a):
                    @pl.when(tab[where[f"part{part}_{a}0"] + s] != 0)
                    def _():
                        pltpu.make_async_copy(some, xr_v.at[a, s], sem_r.at[a, s]).wait()
                        for b in range(B_CNT):
                            n = a * B_CNT + b

                            @pl.when(flag(f"active{a}{b}"))
                            def _(n=n):
                                pltpu.make_async_copy(some, xb.at[n, s], sem_b.at[n, s]).wait()
                                acc[n] -= dot(xr_v[a, s], xb[n, s])

                    return carry

                lax.fori_loop(0, FRONTS, row_step, 0)
            if columns_x:
                def column_step(s, carry):
                    for _ in range(1 + A_CNT):
                        pltpu.make_async_copy(some, xc_v.at[s], sem_c.at[s]).wait()
                    for b in range(B_CNT):
                        @pl.when(tab[where[f"col{b}_0"] + s] != 0)
                        def _(b=b):
                            for a in range(A_CNT):
                                n = a * B_CNT + b

                                @pl.when(flag(f"active{a}{b}"))
                                def _(a=a, n=n):
                                    acc[n] -= dot(xa[a, s], xc_v[s])

                    return carry

                lax.fori_loop(0, FRONTS, column_step, 0)
            if final_c is None:
                outs = [
                    pltpu.make_async_copy(acc.at[n], out.at[a, b], sem_w.at[n])
                    for n, (a, b) in enumerate(tiles_ab)
                ]
                for cp in outs:
                    cp.start()
                for cp in outs:
                    cp.wait()
                return
            pltpu.make_async_copy(at(refs, final_c), x_v, sem_w.at[count]).wait()
            outs = []
            for a in range(A_CNT):
                for b in range(B_CNT):
                    n = a * B_CNT + b

                    @pl.when(flag(f"own{a}{b}"))
                    def _(n=n):
                        acc[n] = x_v[...].astype(F32)

                    for q in range(chunks):
                        out_v[a, :, q * B_CNT + b, :] = acc[n, :, q * lanes : (q + 1) * lanes]
                cp = pltpu.make_async_copy(out_v.at[a], out.at[a], sem_w.at[a])
                cp.start()
                outs.append(cp)
            for cp in outs:
                cp.wait()

        wide = final_x is not None
        out_tile = (A_CNT, nb, chunks * B_CNT, lanes)
        scratch = [
            pltpu.VMEM((count,) + tile, w.dtype),
            pltpu.VMEM((count,) + tile, F32),
            pltpu.VMEM((A_CNT, FRONTS) + tile if columns_x else (1, 1, 8, 128), BF16),
            pltpu.VMEM((count, FRONTS) + tile, BF16),
            pltpu.VMEM((FRONTS,) + tile, BF16),
            pltpu.VMEM((A_CNT, FRONTS) + tile, BF16),
            pltpu.VMEM(tile, BF16),
            pltpu.VMEM(out_tile if wide else (1, 8, 8, 128), F32),
            pltpu.SemaphoreType.DMA((A_CNT, FRONTS)),
            pltpu.SemaphoreType.DMA((count, FRONTS)),
            pltpu.SemaphoreType.DMA((FRONTS,)),
            pltpu.SemaphoreType.DMA((count + 1,)),
        ]
        shape = out_tile if wide else (A_CNT, B_CNT) + tile
        return call(body, kernel, table, jax.ShapeDtypeStruct(shape, F32), scratch, 12 * mm)

    def lagged(x, which):
        down, right = [], []
        for s, lag in which:
            for k, r, c in plan.sources(s):
                if k - lag >= 0:
                    down.append((dev(r, c), dev(r - lag, c)))
                right.append((dev(r, c), dev(r, c + lag)))
        return send(x, down), send(x, right)

    def ring(fronts, x):
        outs = [x]
        src = [p for s in fronts for p in plan.sources(s)]
        for sign, hops in ((1, plan.forward), (-1, plan.backward)):
            v = x
            for h in range(hops):
                at_hop = lambda c, h: plan.ring[(plan.pos[c] + sign * h) % N]
                v = send(v, [(dev(r, at_hop(c, h)), dev(r, at_hop(c, h + 1))) for k, r, c in src])
                outs.append(v)
        return outs

    def column_all(x):
        if not plan.pairs_of_rows:
            return [x] + [
                send(x, [(dev(r + m, c), dev(r, c)) for r in range(R) for c in range(N)])
                for m in range(1, R)
            ]
        places = [(r, c) for r in range(R) for c in range(N)]
        swap = lambda v, m: send(v, [(dev(r, c), dev(r ^ m, c)) for r, c in places])
        other = swap(x, 2)
        return [x, swap(x, 1), other, swap(other, 1)]

    move_a(0)
    move_a(3)
    next_a = send(
        lax.dynamic_index_in_dim(upper_a, a0, 0, False),
        [(dev(r, c), dev(r, c + 1)) for k, r, c in plan.sources(2) if k + 1 < N],
    )
    x0 = solve(0, c_stack, True, [], None)
    col_a, row_a = lagged(x0, [(0, 1)])
    col_e, row_e = lagged(x0, [(0, 2)])
    col_f, row_f = lagged(x0, [(0, 3)])
    x1 = solve(1, c_stack, True, [(0, col_a, row_a)], x0)
    col_b, row_b = lagged(x1, [(1, 1)])
    col_c, row_c = lagged(x1, [(1, 2)])
    move_tall(x1)
    x2 = solve(2, c_stack, True, [(0, col_e, row_e), (1, col_b, row_b)], x1)
    col_d, row_d = lagged(x2, [(2, 1)])
    move_a(2)
    base = older(3, [(0, col_f, row_f), (1, col_c, row_c)])
    x3 = solve(3, base, False, [(2, col_d, row_d)], x2)
    rows_x = ring(range(FRONTS), x3)
    w = update(0, c_stack, early_hops, rows_x, column_all(x3), None)
    w = update(1, w, late_hops, rows_x, [], x3)
    w = w.reshape(A_CNT, nb, w.shape[2] // B_CNT, B_CNT, w.shape[3])
    return jnp.transpose(w, (0, 1, 3, 2, 4)).reshape(right_side.shape)


def solution(mesh):
    return jax.shard_map(
        steps,
        mesh=mesh,
        in_specs=(
            P(None, "row", "col"),
            P(None, "row", None, "col"),
            P(None, "row", None, "col"),
            P(None, "row", None),
            P(None, "col", None),
            P(None, "row"),
            P(None, "col"),
        ),
        out_specs=P(None, "row", None, "col"),
        check_vma=False,
    )
```
